32 devices in a mesh: row: 4 (over z), col: 2 (over x), depth: 4 (over y, core).
Axes of the slice: x: 2, y: 2, z: 4, core: 2. Of those that a mesh axis runs over, the one named last changes fastest.
Arguments:
- pair_input: bfloat16 [192, 192, 128], P('row', ('col', 'depth')), may hold values from -40 to 40
- in_gain: float32 [128], replicated, may hold values from 0.1 to 1.9
- in_shift: float32 [128], replicated, may hold values from -3 to 3
- w_proj: bfloat16 [128, 512], replicated, may hold values from -0.5 to 0.5
- w_gate: bfloat16 [128, 128], replicated, may hold values from -0.5 to 0.5
- out_gain: float32 [128], replicated, may hold values from 0.1 to 1.9
- out_shift: float32 [128], replicated, may hold values from -3 to 3
- w_out: bfloat16 [128, 128], replicated, may hold values from -0.5 to 0.5
Outputs:
- update: bfloat16 [192, 192, 128], P('row', ('col', 'depth'))
The draws below stay inside these ranges and needn't reach their ends.
All inputs are finite; a program needn't handle non-finite values.
Results may differ from the reference program's by a relative error of at most 0.013.
Values may be sent and summed in bfloat16 or wider, within the bound.
A program may use at most 64 MiB of HBM per device.

```python
import math
import jax
import jax.numpy as jnp
from jax import lax

C_Z = 128
C = 128
RESIDUES = 192


def draw_pair_input(key, part):
    key_entries = jax.random.fold_in(key, 11)
    key_scales = jax.random.fold_in(key, 12)
    scales = jnp.exp(jax.random.uniform(key_scales, (RESIDUES, RESIDUES, 1), jnp.float32, 0.0, math.log(10.0)))
    entries = jnp.clip(jax.random.normal(key_entries, (RESIDUES, RESIDUES, C_Z), jnp.float32), -4.0, 4.0)
    values = entries * scales
    return values.astype(jnp.bfloat16)


def gaussian(stream_key, shape, width, most, kind=jnp.bfloat16):
    return jnp.clip(width * jax.random.normal(stream_key, shape, jnp.float32), -most, most).astype(kind)


def setup_inputs(seed: int = 0) -> dict:
    splits = jax.random.split(jax.random.key(seed), 9)
    return {
        "pair_input": draw_pair_input(jax.random.fold_in(splits[8], 71), 0),
        "in_gain": jnp.clip(1.0 + 0.18 * jax.random.normal(splits[1], (C_Z,), jnp.float32), 0.1, 1.9),
        "in_shift": gaussian(splits[2], (C_Z,), 0.5, 3.0, jnp.float32),
        "w_proj": gaussian(splits[3], (C_Z, 4 * C), C_Z ** -0.5, 0.5),
        "w_gate": gaussian(splits[4], (C_Z, C_Z), C_Z ** -0.5, 0.5),
        "out_gain": jnp.clip(1.0 + 0.18 * jax.random.normal(splits[5], (C,), jnp.float32), 0.1, 1.9),
        "out_shift": gaussian(splits[6], (C,), 0.5, 3.0, jnp.float32),
        "w_out": gaussian(splits[7], (C, C_Z), C ** -0.5, 0.5),
    }


def layer_norm(values, scaling, offsets):
    average = lax.optimization_barrier(jnp.mean(values, axis=-1, keepdims=True))
    centred = values - average
    variance = lax.optimization_barrier(jnp.mean(centred * centred, axis=-1, keepdims=True))
    return centred * lax.rsqrt(variance + 1e-05) * scaling + offsets

def reference(pair_input, in_gain, in_shift, w_proj, w_gate, out_gain, out_shift, w_out):
    normed = layer_norm(pair_input.astype(jnp.float32), in_gain, in_shift).astype(jnp.bfloat16)
    channels = w_proj.shape[1] // 4

    def side_rows(normed_row):
        projected = jnp.dot(normed_row, w_proj, preferred_element_type=jnp.float32)
        left_side = (jax.nn.sigmoid(projected[:, :channels]) * projected[:, channels:2 * channels]).astype(jnp.bfloat16)
        right_side = (jax.nn.sigmoid(projected[:, 2 * channels:3 * channels]) * projected[:, 3 * channels:]).astype(jnp.bfloat16)
        return (left_side, right_side)
    left_side, right_side = lax.map(side_rows, normed)
    product = jnp.einsum('kic,kjc->ijc', left_side.astype(jnp.float32), right_side.astype(jnp.float32), precision=lax.Precision.HIGHEST)
    product_norm = layer_norm(product, out_gain, out_shift).astype(jnp.bfloat16)
    gating = jax.nn.sigmoid(jnp.einsum('xyc,cd->xyd', normed.astype(jnp.float32), w_gate.astype(jnp.float32), precision=lax.Precision.HIGHEST))
    projected_out = jnp.einsum('xyc,cd->xyd', product_norm.astype(jnp.float32), w_out.astype(jnp.float32), precision=lax.Precision.HIGHEST)
    return (gating * projected_out).astype(jnp.bfloat16)
```

```python
import functools

import jax
import jax.numpy as jnp
from jax import lax
from jax.experimental import pallas as pl
from jax.experimental.pallas import tpu as pltpu
from jax.sharding import PartitionSpec as P

F32 = jnp.float32
BF16 = jnp.bfloat16
LANES = 128
SUB = 8


def dot(a, b, ca, cb):
    return lax.dot_general(a, b, (((ca,), (cb,)), ((), ())), preferred_element_type=F32)


def kernel(
    sizes,
    x_ref,
    in_gain_ref,
    in_shift_ref,
    w_proj_ref,
    w_gate_ref,
    out_gain_ref,
    out_shift_ref,
    w_out_ref,
    out_ref,
    normed,
    w_turned,
    gating,
    packed,
    send1,
    recv1,
    gathered,
    left_wide,
    right_wide,
    planes,
    flat,
    packed2,
    send2,
    recv2,
    gathered2,
    send_sem1,
    recv_sem1,
    send_sem2,
    recv_sem2,
):
    rows, cols, depths = sizes
    others = cols * depths
    count = rows * others
    local_k, local_i, width = x_ref.shape
    hidden = w_out_ref.shape[0]
    own = hidden // count
    groups = local_i // SUB
    blocks = local_k // local_i
    pairs = blocks // 2
    tiles = pairs * groups * groups
    span1 = 2 * own * tiles
    padded = packed2.shape[0] // hidden
    span2 = own * padded
    line = groups * others

    my_row = lax.axis_index("row")
    my_other = lax.axis_index("col") * depths + lax.axis_index("depth")
    me = my_row * others + my_other

    def device(p):
        q = lax.rem(p, others)
        return (lax.div(p, others), lax.div(q, depths), lax.rem(q, depths))

    barrier = pltpu.get_barrier_semaphore()

    def greet(d, carry):
        pl.semaphore_signal(
            barrier, inc=1, device_id=device(lax.rem(me + d, count)), device_id_type=pl.DeviceIdType.MESH
        )
        return carry

    lax.fori_loop(1, count, greet, 0)

    values = x_ref[...].astype(F32)
    centred = values - jnp.mean(values, axis=-1, keepdims=True)
    variance = jnp.mean(centred * centred, axis=-1, keepdims=True)
    normed[...] = (
        centred * lax.rsqrt(variance + 1e-05) * in_gain_ref[...].reshape(1, 1, width)
        + in_shift_ref[...].reshape(1, 1, width)
    )
    w_turned[...] = w_proj_ref[...].astype(F32).T.astype(BF16)

    def tile_parts(t):
        pair, rest = t // (groups * groups), t % (groups * groups)
        return pair, rest // groups, rest % groups

    for t in range(tiles):
        pair, first, second = tile_parts(t)
        parts = [
            normed[
                pl.ds((2 * pair + b) * local_i + first * SUB, SUB), pl.ds(second * SUB, SUB), :
            ].reshape(SUB * SUB, width)
            for b in range(2)
        ]
        block = jnp.concatenate(parts, axis=0).astype(BF16)
        projected = dot(w_turned[...], block, 1, 1)
        for side in range(2):
            start = 2 * side * hidden
            gated = (
                jax.nn.sigmoid(projected[start : start + hidden])
                * projected[start + hidden : start + 2 * hidden]
            )
            packed[pl.ds(side * tiles + t, hidden, stride=2 * tiles), :] = gated
        gating[t] = jax.nn.sigmoid(dot(block, w_gate_ref[...], 1, 0))

    def pack1(p, carry):
        send1[p] = packed[pl.ds(pl.multiple_of(p * span1, SUB), span1), :].astype(BF16)
        return carry

    lax.fori_loop(0, count, pack1, 0)
    pl.semaphore_wait(barrier, count - 1)

    def copy1(p, slot):
        return pltpu.make_async_remote_copy(
            src_ref=send1.at[p],
            dst_ref=recv1.at[slot],
            send_sem=send_sem1.at[p],
            recv_sem=recv_sem1.at[slot],
            device_id=device(p),
            device_id_type=pl.DeviceIdType.MESH,
        )

    def copy2(p, slot):
        return pltpu.make_async_remote_copy(
            src_ref=send2.at[p],
            dst_ref=recv2.at[slot],
            send_sem=send_sem2.at[p],
            recv_sem=recv_sem2.at[slot],
            device_id=device(p),
            device_id_type=pl.DeviceIdType.MESH,
        )

    def start1(d, carry):
        copy1(lax.rem(me + d, count), me).start()
        return carry

    lax.fori_loop(1, count, start1, 0)

    gathered[pl.ds(pl.multiple_of(me * span1, SUB), span1), :] = send1[me].astype(F32)

    def take1(d, carry):
        p = lax.rem(me + count - d, count)
        copy1(p, p).wait_recv()
        gathered[pl.ds(pl.multiple_of(p * span1, SUB), span1), :] = recv1[p].astype(F32)
        return carry

    lax.fori_loop(1, count, take1, 0)

    lane_row = lax.broadcasted_iota(jnp.int32, (LANES, LANES), 0)
    lane_col = lax.broadcasted_iota(jnp.int32, (LANES, LANES), 1)
    same_k = lane_row // SUB == lane_col // SUB
    spread = jnp.concatenate(
        [jnp.where(same_k & (lane_row % SUB == j), 1.0, 0.0) for j in range(SUB)], axis=1
    ).astype(BF16)
    lane_of = lax.broadcasted_iota(jnp.int32, (line, LANES), 1)
    zero = jnp.zeros((line, LANES), F32)
    total = SUB * line
    for c in range(own):

        def fill(step, carry, c=c):
            r = lax.div(step, pairs * groups)
            part = lax.rem(step, pairs * groups)

            def side_block(side):
                start = r * others * span1 + (c * 2 + side) * tiles + part * groups
                return jnp.concatenate(
                    [gathered[pl.ds(start + g, others, stride=span1), :] for g in range(groups)], axis=0
                )

            left = side_block(0)
            right = dot(side_block(1).astype(BF16), spread, 1, 0)
            lanes = pl.ds(pl.multiple_of(step * LANES, LANES), LANES)
            left_wide[:, lanes] = jnp.concatenate(
                [jnp.where(lane_of % SUB == i, left, zero) for i in range(SUB)], axis=0
            ).astype(BF16)
            right_wide[:, lanes] = jnp.concatenate(
                [right[:, j * LANES : (j + 1) * LANES] for j in range(SUB)], axis=0
            ).astype(BF16)
            return carry

        lax.fori_loop(0, rows * pairs * groups, fill, 0, unroll=rows * pairs * groups <= 16)
        planes[pl.ds(c * total, total), :] = dot(left_wide[...], right_wide[...], 1, 1).astype(BF16)

    row_of = lax.broadcasted_iota(jnp.int32, (total, LANES), 0)
    col_of = lax.broadcasted_iota(jnp.int32, (total, LANES), 1)
    same_j = row_of // line == col_of % SUB
    row_group = row_of % line

    def flatten(g, carry):
        picker = jnp.where(same_j & (row_group == g), 1.0, 0.0).astype(BF16)
        for c in range(own):
            wide = dot(planes[pl.ds(c * total, total), :], picker, 1, 0)
            kept = wide[:line]
            for i in range(1, SUB):
                kept = jnp.where((lane_of // SUB) % SUB == i, wide[i * line : (i + 1) * line], kept)
            flat[pl.ds(pl.multiple_of((c * line + g) * line, SUB), line), :] = kept
        return carry

    lax.fori_loop(0, line, flatten, 0, unroll=2)

    lane_half = lax.broadcasted_iota(jnp.int32, (others, LANES), 1) < LANES // 2
    for c in range(own):
        for t in range(tiles):
            pair, first, second = tile_parts(t)
            for r in range(rows):
                start = (c * line + second * others) * line + first * others + r * blocks + 2 * pair
                even = flat[pl.ds(start, others, stride=line), :]
                odd = flat[pl.ds(start + 1, others, stride=line), :]
                packed2[pl.ds(r * others * span2 + c * padded + t, others, stride=span2), :] = jnp.where(
                    lane_half, even, odd
                )

    def pack2(p, carry):
        send2[p] = packed2[pl.ds(pl.multiple_of(p * span2, SUB), span2), :].astype(BF16)
        return carry

    lax.fori_loop(0, count, pack2, 0)

    def start2(d, carry):
        copy2(lax.rem(me + d, count), me).start()
        return carry

    lax.fori_loop(1, count, start2, 0)
    out_gain = jnp.broadcast_to(out_gain_ref[...].reshape(1, hidden), (LANES, hidden)).T
    out_shift = jnp.broadcast_to(out_shift_ref[...].reshape(1, hidden), (LANES, hidden)).T
    gathered2[pl.ds(pl.multiple_of(me * span2, SUB), span2), :] = send2[me].astype(F32)

    def take2(d, carry):
        p = lax.rem(me + count - d, count)
        copy2(p, p).wait_recv()
        gathered2[pl.ds(pl.multiple_of(p * span2, SUB), span2), :] = recv2[p].astype(F32)
        return carry

    lax.fori_loop(1, count, take2, 0)

    for t in range(tiles):
        pair, first, second = tile_parts(t)
        product = gathered2[pl.ds(t, hidden, stride=padded), :]
        spread_out = product - jnp.mean(product, axis=0, keepdims=True)
        moment = jnp.mean(spread_out * spread_out, axis=0, keepdims=True)
        product_norm = (spread_out * lax.rsqrt(moment + 1e-05) * out_gain + out_shift).astype(BF16)
        update = (gating[t] * dot(product_norm, w_out_ref[...], 0, 0)).astype(BF16)
        for b in range(2):
            out_ref[
                pl.ds((2 * pair + b) * local_i + first * SUB, SUB), pl.ds(second * SUB, SUB), :
            ] = update[b * SUB * SUB : (b + 1) * SUB * SUB].reshape(SUB, SUB, width)

    def finish(d, carry):
        p = lax.rem(me + d, count)
        copy1(p, me).wait_send()
        copy2(p, me).wait_send()
        return carry

    lax.fori_loop(1, count, finish, 0)


def per_device(sizes, pair_input, in_gain, in_shift, w_proj, w_gate, out_gain, out_shift, w_out):
    rows, cols, depths = sizes
    others = cols * depths
    count = rows * others
    local_k, local_i, width = pair_input.shape
    hidden = w_out.shape[0]
    own = hidden // count
    residues = local_k * rows
    tiles = local_k * local_i // LANES
    span1 = 2 * own * tiles
    padded = tiles
    while (own * padded) % SUB:
        padded += 1
    span2 = own * padded
    line = residues // SUB
    deep = residues * SUB
    vmem = pl.BlockSpec(memory_space=pltpu.VMEM)
    return pl.pallas_call(
        functools.partial(kernel, sizes),
        out_shape=jax.ShapeDtypeStruct(pair_input.shape, BF16),
        in_specs=[vmem] * 8,
        out_specs=vmem,
        scratch_shapes=[
            pltpu.VMEM(pair_input.shape, F32),
            pltpu.VMEM(w_proj.shape[::-1], BF16),
            pltpu.VMEM((tiles, LANES, width), F32),
            pltpu.VMEM((hidden * 2 * tiles, LANES), F32),
            pltpu.VMEM((count, span1, LANES), BF16),
            pltpu.VMEM((count, span1, LANES), BF16),
            pltpu.VMEM((count * span1, LANES), F32),
            pltpu.VMEM((residues, deep), BF16),
            pltpu.VMEM((residues, deep), BF16),
            pltpu.VMEM((own * residues, residues), BF16),
            pltpu.VMEM((own * line * line, LANES), F32),
            pltpu.VMEM((hidden * padded, LANES), F32),
            pltpu.VMEM((count, span2, LANES), BF16),
            pltpu.VMEM((count, span2, LANES), BF16),
            pltpu.VMEM((hidden * padded, LANES), F32),
            pltpu.SemaphoreType.DMA((count,)),
            pltpu.SemaphoreType.DMA((count,)),
            pltpu.SemaphoreType.DMA((count,)),
            pltpu.SemaphoreType.DMA((count,)),
        ],
        compiler_params=pltpu.CompilerParams(
            collective_id=0, has_side_effects=True, vmem_limit_bytes=60 * 1024 * 1024
        ),
    )(
        pair_input,
        in_gain.reshape(1, -1),
        in_shift.reshape(1, -1),
        w_proj,
        w_gate,
        out_gain.reshape(1, -1),
        out_shift.reshape(1, -1),
        w_out,
    )


def solution(mesh):
    sizes = (mesh.shape["row"], mesh.shape["col"], mesh.shape["depth"])
    placed = (P("row", ("col", "depth"), None), P(), P(), P(), P(), P(), P(), P())
    return jax.shard_map(
        functools.partial(per_device, sizes),
        mesh=mesh,
        in_specs=placed,
        out_specs=P("row", ("col", "depth"), None),
        check_vma=False,
    )
```

```python
import functools

import jax
import jax.numpy as jnp
from jax import lax
from jax.experimental import pallas as pl
from jax.experimental.pallas import tpu as pltpu
from jax.sharding import PartitionSpec as P

F32 = jnp.float32
BF16 = jnp.bfloat16
LANES = 128
SUB = 8
HALVES = 1


def padded_rows(needed, channels):
    while (needed * channels) % SUB:
        needed += 1
    return needed


def dot(a, b, ca, cb):
    return lax.dot_general(a, b, (((ca,), (cb,)), ((), ())), preferred_element_type=F32)


def kernel(
    sizes,
    x_ref,
    in_gain_ref,
    in_shift_ref,
    w_proj_ref,
    w_gate_ref,
    out_gain_ref,
    out_shift_ref,
    w_out_ref,
    out_ref,
    normed,
    w_turned,
    gating,
    packed,
    send1,
    recv1,
    gathered,
    left_wide,
    right_wide,
    planes,
    flat,
    packed2,
    send2,
    recv2,
    gathered2,
    spread,
    picker,
    send_sem1,
    recv_sem1,
    send_sem2,
    recv_sem2,
):
    rows, cols, depths = sizes
    others = cols * depths
    count = rows * others
    local_k, local_i, width = x_ref.shape
    hidden = w_out_ref.shape[0]
    own = hidden // count
    groups = local_i // SUB
    blocks = local_k // local_i
    pairs = blocks // 2
    tiles = pairs * groups * groups
    halves = send1.shape[0]
    own_half = own // halves
    part_hidden = hidden // halves
    padded1 = packed.shape[0] // hidden
    padded2 = packed2.shape[0] // hidden
    span1 = own_half * padded1
    span2 = own_half * padded2
    line = groups * others

    my_row = lax.axis_index("row")
    my_other = lax.axis_index("col") * depths + lax.axis_index("depth")
    me = my_row * others + my_other

    def device(p):
        q = lax.rem(p, others)
        return (lax.div(p, others), lax.div(q, depths), lax.rem(q, depths))

    barrier = pltpu.get_barrier_semaphore()

    def greet(d, carry):
        pl.semaphore_signal(
            barrier, inc=1, device_id=device(lax.rem(me + d, count)), device_id_type=pl.DeviceIdType.MESH
        )
        return carry

    lax.fori_loop(1, count, greet, 0)

    values = x_ref[...].astype(F32)
    centred = values - jnp.mean(values, axis=-1, keepdims=True)
    variance = jnp.mean(centred * centred, axis=-1, keepdims=True)
    normed[...] = (
        centred * lax.rsqrt(variance + 1e-05) * in_gain_ref[...].reshape(1, 1, width)
        + in_shift_ref[...].reshape(1, 1, width)
    )
    w_turned[...] = w_proj_ref[...].astype(F32).T.astype(BF16)

    def tile_parts(t):
        pair, rest = t // (groups * groups), t % (groups * groups)
        return pair, rest // groups, rest % groups

    def tile_block(t):
        pair, first, second = tile_parts(t)
        parts = [
            normed[
                pl.ds((2 * pair + b) * local_i + first * SUB, SUB), pl.ds(second * SUB, SUB), :
            ].reshape(SUB * SUB, width)
            for b in range(2)
        ]
        return jnp.concatenate(parts, axis=0).astype(BF16)

    def project(h):
        for t in range(tiles):
            block = tile_block(t)
            for side in range(2):
                start = 2 * side * hidden + h * part_hidden
                gates = dot(w_turned[pl.ds(start, part_hidden), :], block, 1, 1)
                edges = dot(w_turned[pl.ds(start + hidden, part_hidden), :], block, 1, 1)
                packed[
                    pl.ds(h * part_hidden * padded1 + side * tiles + t, part_hidden, stride=padded1), :
                ] = jax.nn.sigmoid(gates) * edges

        def pack1(p, carry):
            start = pl.multiple_of((h * count + p) * span1, SUB)
            send1[h, p] = packed[pl.ds(start, span1), :].astype(BF16)
            return carry

        lax.fori_loop(0, count, pack1, 0, unroll=4)

    def copy1(h, p, slot):
        return pltpu.make_async_remote_copy(
            src_ref=send1.at[h, p],
            dst_ref=recv1.at[h, slot],
            send_sem=send_sem1.at[h, p],
            recv_sem=recv_sem1.at[h, slot],
            device_id=device(p),
            device_id_type=pl.DeviceIdType.MESH,
        )

    def copy2(h, p, slot):
        return pltpu.make_async_remote_copy(
            src_ref=send2.at[h, p],
            dst_ref=recv2.at[h, slot],
            send_sem=send_sem2.at[h, p],
            recv_sem=recv_sem2.at[h, slot],
            device_id=device(p),
            device_id_type=pl.DeviceIdType.MESH,
        )

    def peer(d):
        return lax.rem(me + d, count)

    for h in range(halves):
        project(h)
        if h == 0:
            pl.semaphore_wait(barrier, count - 1)

        def start1(d, carry, h=h):
            copy1(h, peer(d), me).start()
            return carry

        lax.fori_loop(1, count, start1, 0)

    for t in range(tiles):
        gating[t] = jax.nn.sigmoid(dot(tile_block(t), w_gate_ref[...], 1, 0))
    lane_row = lax.broadcasted_iota(jnp.int32, (LANES, LANES), 0)
    lane_col = lax.broadcasted_iota(jnp.int32, (LANES, LANES), 1)
    same_k = lane_row // SUB == lane_col // SUB
    for j in range(SUB):
        spread[:, j * LANES : (j + 1) * LANES] = jnp.where(
            same_k & (lane_row % SUB == j), 1.0, 0.0
        ).astype(BF16)
    total = SUB * line
    row_of = lax.broadcasted_iota(jnp.int32, (total, 2 * LANES), 0)
    col_of = lax.broadcasted_iota(jnp.int32, (total, 2 * LANES), 1)
    same_j = row_of // line == col_of % SUB
    row_group = row_of % line
    half_line = others // 2
    second_half = jnp.where(col_of % LANES < LANES // 2, 0, half_line)
    hoisted = picker.shape[0] == line // 4

    def group_of(pair):
        return lax.div(pair, half_line) * others + lax.rem(pair, half_line)

    def fill_picker(g, slot):
        wanted = jnp.where(col_of < LANES, group_of(2 * g), group_of(2 * g + 1)) + second_half
        picker[slot] = jnp.where(same_j & (row_group == wanted), 1.0, 0.0).astype(BF16)

    if hoisted:

        def hoist(g, carry):
            fill_picker(g, g)
            return carry

        lax.fori_loop(0, line // 4, hoist, 0)
    lane_of = lax.broadcasted_iota(jnp.int32, (line, LANES), 1)
    lane_half = lax.broadcasted_iota(jnp.int32, (others, LANES), 1) < LANES // 2
    zero = jnp.zeros((line, LANES), F32)
    wide_of = lax.broadcasted_iota(jnp.int32, (line, 2 * LANES), 1)
    odd_row = lax.broadcasted_iota(jnp.int32, (line, LANES), 0) % 2 == 1
    steps = rows * pairs * groups
    batch = max(n for n in range(1, steps + 1) if steps % n == 0 and (n * line <= 288 or n == 1))

    def middle(h):
        base = h * count * span1
        start = pl.multiple_of(base + me * span1, SUB)
        gathered[pl.ds(start, span1), :] = send1[h, me].astype(F32)

        def take1(d, carry):
            p = lax.rem(me + count - d, count)
            copy1(h, p, p).wait_recv()
            start = pl.multiple_of(base + p * span1, SUB)
            gathered[pl.ds(start, span1), :] = recv1[h, p].astype(F32)
            return carry

        lax.fori_loop(1, count, take1, 0)
        for c in range(own_half):

            def fill(turn, carry, c=c):
                rights = []
                for n in range(batch):
                    step = turn * batch + n
                    r = lax.div(step, pairs * groups)
                    part = lax.rem(step, pairs * groups)
                    start = base + r * others * span1 + c * padded1 + part * groups
                    left = jnp.concatenate(
                        [gathered[pl.ds(start + g, others, stride=span1), :] for g in range(groups)],
                        axis=0,
                    )
                    rights += [
                        gathered[pl.ds(start + tiles + g, others, stride=span1), :]
                        for g in range(groups)
                    ]
                    lanes = pl.ds(pl.multiple_of(step * LANES, LANES), LANES)
                    left_wide[:, lanes] = jnp.concatenate(
                        [jnp.where(lane_of % SUB == i, left, zero) for i in range(SUB)], axis=0
                    ).astype(BF16)
                right = dot(jnp.concatenate(rights, axis=0).astype(BF16), spread[...], 1, 0)
                for n in range(batch):
                    lanes = pl.ds(pl.multiple_of((turn * batch + n) * LANES, LANES), LANES)
                    right_wide[:, lanes] = jnp.concatenate(
                        [
                            right[n * line : (n + 1) * line, j * LANES : (j + 1) * LANES]
                            for j in range(SUB)
                        ],
                        axis=0,
                    ).astype(BF16)
                return carry

            if steps == batch:
                fill(0, 0)
            else:
                lax.fori_loop(0, steps // batch, fill, 0)
            planes[pl.ds(c * total, total), :] = dot(left_wide[...], right_wide[...], 1, 1).astype(BF16)

        def flatten(g, carry):
            slot = g if hoisted else 0
            if not hoisted:
                fill_picker(g, 0)
            for c in range(own_half):
                wide = dot(planes[pl.ds(c * total, total), :], picker[slot], 1, 0)
                kept = wide[:line]
                for i in range(1, SUB):
                    kept = jnp.where((wide_of // SUB) % SUB == i, wide[i * line : (i + 1) * line], kept)
                for n in range(2):
                    mine = kept[:, n * LANES : (n + 1) * LANES]
                    turned = pltpu.roll(mine, LANES // 2, 1)
                    group = group_of(2 * g + n)
                    low = pl.multiple_of((c * line + group) * line, SUB)
                    high = pl.multiple_of((c * line + group + half_line) * line, SUB)
                    flat[pl.ds(low, line), :] = jnp.where(odd_row, turned, mine)
                    flat[pl.ds(high, line), :] = jnp.where(odd_row, mine, turned)
            return carry

        lax.fori_loop(0, line // 4, flatten, 0, unroll=2)
        for c in range(own_half):
            for t in range(tiles):
                pair, first, second = tile_parts(t)
                for r in range(rows):
                    start = (c * line + second * others) * line + first * others + r * blocks + 2 * pair
                    even = flat[pl.ds(start, others, stride=line), :]
                    odd = flat[pl.ds(start + 1, others, stride=line), :]
                    packed2[
                        pl.ds((h * count + r * others) * span2 + c * padded2 + t, others, stride=span2), :
                    ] = jnp.where(lane_half, even, odd)

        def pack2(p, carry):
            start = pl.multiple_of((h * count + p) * span2, SUB)
            send2[h, p] = packed2[pl.ds(start, span2), :].astype(BF16)
            return carry

        lax.fori_loop(0, count, pack2, 0, unroll=4)

        def start2(d, carry):
            copy2(h, peer(d), me).start()
            return carry

        lax.fori_loop(1, count, start2, 0)

    for h in range(halves):
        middle(h)
    out_gain = jnp.broadcast_to(out_gain_ref[...].reshape(1, hidden), (LANES, hidden)).T
    out_shift = jnp.broadcast_to(out_shift_ref[...].reshape(1, hidden), (LANES, hidden)).T
    for h in range(halves):
        start = pl.multiple_of((h * count + me) * span2, SUB)
        gathered2[pl.ds(start, span2), :] = send2[h, me].astype(F32)

        def take2(d, carry, h=h):
            p = lax.rem(me + count - d, count)
            copy2(h, p, p).wait_recv()
            start = pl.multiple_of((h * count + p) * span2, SUB)
            gathered2[pl.ds(start, span2), :] = recv2[h, p].astype(F32)
            return carry

        lax.fori_loop(1, count, take2, 0)

    for t in range(tiles):
        pair, first, second = tile_parts(t)
        product = gathered2[pl.ds(t, hidden, stride=padded2), :]
        spread_out = product - jnp.mean(product, axis=0, keepdims=True)
        moment = jnp.mean(spread_out * spread_out, axis=0, keepdims=True)
        product_norm = (spread_out * lax.rsqrt(moment + 1e-05) * out_gain + out_shift).astype(BF16)
        update = (gating[t] * dot(product_norm, w_out_ref[...], 0, 0)).astype(BF16)
        for b in range(2):
            out_ref[
                pl.ds((2 * pair + b) * local_i + first * SUB, SUB), pl.ds(second * SUB, SUB), :
            ] = update[b * SUB * SUB : (b + 1) * SUB * SUB].reshape(SUB, SUB, width)

    def finish(d, carry):
        p = lax.rem(me + d, count)
        for h in range(halves):
            copy1(h, p, me).wait_send()
            copy2(h, p, me).wait_send()
        return carry

    lax.fori_loop(1, count, finish, 0)


def per_device(sizes, pair_input, in_gain, in_shift, w_proj, w_gate, out_gain, out_shift, w_out):
    rows, cols, depths = sizes
    others = cols * depths
    count = rows * others
    local_k, local_i, width = pair_input.shape
    hidden = w_out.shape[0]
    own = hidden // count
    residues = local_k * rows
    tiles = local_k * local_i // LANES
    halves = HALVES if own % HALVES == 0 else 1
    own_half = own // halves
    padded1 = padded_rows(2 * tiles, own_half)
    padded2 = padded_rows(tiles, own_half)
    span1 = own_half * padded1
    span2 = own_half * padded2
    line = residues // SUB
    deep = residues * SUB
    pickers = line // 4 if residues * line * LANES <= 1 << 20 else 1
    vmem = pl.BlockSpec(memory_space=pltpu.VMEM)
    return pl.pallas_call(
        functools.partial(kernel, sizes),
        out_shape=jax.ShapeDtypeStruct(pair_input.shape, BF16),
        in_specs=[vmem] * 8,
        out_specs=vmem,
        scratch_shapes=[
            pltpu.VMEM(pair_input.shape, F32),
            pltpu.VMEM(w_proj.shape[::-1], BF16),
            pltpu.VMEM((tiles, LANES, width), F32),
            pltpu.VMEM((hidden * padded1, LANES), F32),
            pltpu.VMEM((halves, count, span1, LANES), BF16),
            pltpu.VMEM((halves, count, span1, LANES), BF16),
            pltpu.VMEM((hidden * padded1, LANES), F32),
            pltpu.VMEM((residues, deep), BF16),
            pltpu.VMEM((residues, deep), BF16),
            pltpu.VMEM((own_half * residues, residues), BF16),
            pltpu.VMEM((own_half * line * line, LANES), F32),
            pltpu.VMEM((hidden * padded2, LANES), F32),
            pltpu.VMEM((halves, count, span2, LANES), BF16),
            pltpu.VMEM((halves, count, span2, LANES), BF16),
            pltpu.VMEM((hidden * padded2, LANES), F32),
            pltpu.VMEM((LANES, SUB * LANES), BF16),
            pltpu.VMEM((pickers, residues, 2 * LANES), BF16),
            pltpu.SemaphoreType.DMA((halves, count)),
            pltpu.SemaphoreType.DMA((halves, count)),
            pltpu.SemaphoreType.DMA((halves, count)),
            pltpu.SemaphoreType.DMA((halves, count)),
        ],
        compiler_params=pltpu.CompilerParams(
            collective_id=0, has_side_effects=True, vmem_limit_bytes=67_000_000
        ),
    )(
        pair_input,
        in_gain.reshape(1, -1),
        in_shift.reshape(1, -1),
        w_proj,
        w_gate,
        out_gain.reshape(1, -1),
        out_shift.reshape(1, -1),
        w_out,
    )


def solution(mesh):
    sizes = (mesh.shape["row"], mesh.shape["col"], mesh.shape["depth"])
    placed = (P("row", ("col", "depth"), None), P(), P(), P(), P(), P(), P(), P())
    return jax.shard_map(
        functools.partial(per_device, sizes),
        mesh=mesh,
        in_specs=placed,
        out_specs=P("row", ("col", "depth"), None),
        check_vma=False,
    )
```
